128 devices in a mesh: blk: 64 (over x, z, y_lo, core), ep: 2 (over y_hi).
Axes of the slice: x: 4, y: 4 (y_hi: 2, y_lo: 2; y = y_hi * 2 + y_lo), z: 4, core: 2. Of those that a mesh axis runs over, the one named last changes fastest.
Arguments:
- hidden_in: bfloat16 [1024, 4096], P('blk'), may hold values from -6 to 6
- out_grad: bfloat16 [1024, 4096], P('blk'), may hold values from -6 to 6
- expert_ids: int32 [1024, 2], P('blk'), may hold values from 0 to 3, all different within a row; in each aligned block of 16 rows (0 to 15, 16 to 31, ...) at most 12 rows name the same one
- gate_values: bfloat16 [1024, 2], P('blk'), may hold values from 0.099609375 to 1
- w_gate: bfloat16 [4, 14336, 4096], P('ep', 'blk'), may hold values from -0.09375 to 0.09375
- w_up: bfloat16 [4, 14336, 4096], P('ep', 'blk'), may hold values from -0.09375 to 0.09375
- w_down: bfloat16 [4, 14336, 4096], P('ep', 'blk'), may hold values from -0.046875 to 0.046875
Outputs:
- input_grad: bfloat16 [1024, 4096], P('blk')
- gate_grad: float32 [1024, 2], P('blk')
- grad_gate: bfloat16 [4, 14336, 4096], P('ep', 'blk')
- grad_up: bfloat16 [4, 14336, 4096], P('ep', 'blk')
- grad_down: bfloat16 [4, 14336, 4096], P('ep', 'blk')
The draws below stay inside these ranges and needn't reach their ends.
Inputs may be any that keep to these rules, and one draw needn't show every extreme that they name: `expert_ids`: each row names 2 different experts; in each aligned block of 16 rows (the rows of one device) no expert is named by more than 12 rows, a bound that some block reaches.
All inputs are finite; a program needn't handle non-finite values.
Results may differ from the reference program's by a relative error of at most 0.008.
Values may be sent and summed in bfloat16 or wider, within the bound.
No kernel may reach another device: no remote copies, remote signals or barrier semaphores. Data moves between devices by JAX's collectives and lax.ppermute only.
A program may use at most 256 MiB of HBM per device.

```python
import math
import jax
import jax.numpy as jnp
import numpy as np
from jax import lax

D = 4096
FF = 14336
TOP = 2
TOK_DEV = 16
EXPERTS = 4
CAP = 12
TOKENS = 1024


def block_scale(own_key, shape, split, low, largest):
    loudness, own = 1.0, jax.random.fold_in(own_key, 6)
    for dim, blocks in split:
        steps = jnp.exp(jax.random.uniform(jax.random.fold_in(own, dim), (blocks,), jnp.float32, low / len(split), largest / len(split)))
        loudness = loudness * jnp.repeat(steps, shape[dim] // blocks).reshape([-1 if axis == dim else 1 for axis in range(len(shape))])
    return loudness


def shared_out(rng, own, number, rows, count, top, most, lean):
    sequence = jax.random.permutation(rng, count)
    crowded, usual = portions_of(count, rows * top, most, lean, True), portions_of(count, rows * top, most, lean, False)
    places = jnp.arange(count)

    def named(lengths, offset_by):
        used = int((lengths > 0).sum())
        fixed = max(1, used // 4)
        passed = fixed + (places - fixed + offset_by * (used - fixed)) % max(1, count - fixed)
        return jnp.zeros((count,), jnp.int32).at[sequence[jnp.where(places < fixed, places, passed)]].set(jnp.asarray(lengths, jnp.int32))

    lengths = jnp.where(number % 4 == 0, named(crowded, number // 4), named(usual, number - number // 4 - 1))
    mixed = jax.random.permutation(jax.random.fold_in(own, 3), count)
    giver, sink = mixed[0:count // 2 * 2:2], mixed[1:count // 2 * 2:2]
    margin = jnp.minimum(lengths[giver] - 1, most - lengths[sink]) // 2
    margin = jnp.where((giver == sequence[0]) | (sink == sequence[0]) | (lengths[sink] == 0), 0, jnp.maximum(margin, 0))
    passed = jax.random.randint(jax.random.fold_in(own, 4), (count // 2,), 0, 1 << 20) % (margin + 1)
    lengths = lengths.at[giver].add(-passed).at[sink].add(passed)
    items = jnp.searchsorted(jnp.cumsum(lengths), jnp.arange(rows * top), side="right").astype(jnp.int32)
    table = items.reshape(top, rows).T
    table = table[jax.random.permutation(jax.random.fold_in(own, 1), rows)]
    offset_by = jax.random.randint(jax.random.fold_in(own, 2), (rows, 1), 0, top)
    return jnp.take_along_axis(table, (jnp.arange(top)[None, :] + offset_by) % top, axis=1)


def portions_of(number_of, total, bound, slope, full):
    loads = [(1 << 20) // math.isqrt(standing ** slope) + 1 for standing in range(1, number_of + 1)]
    largest = bound if full else min(bound, max(-(-total // number_of), total * loads[0] // sum(loads)))
    least = 1 if total - largest >= number_of - 1 else 0
    given, spare = [largest] + [least] * (number_of - 1), total - largest - least * (number_of - 1)
    while spare > 0:
        free = [i for i in range(1, number_of) if given[i] < largest] or [i for i in range(1, number_of) if given[i] < bound]
        mass, left = sum([loads[i] for i in free]), spare
        for i in free:
            addition = min(bound - given[i], max(1, left * loads[i] // mass), spare)
            given[i] = given[i] + addition
            spare = spare - addition
    return np.array(given)


def scatter_about(rng, extent, scale, bound, cuts=(), held_as=jnp.bfloat16):
    values = jax.random.normal(rng, extent, jnp.float32) * scale
    if len(cuts) > 0:
        values = block_scale(rng, extent, cuts, -0.22, 0.18) * values
    return jnp.clip(values, min=-bound, max=bound).astype(held_as)


def setup_inputs(seed: int = 0) -> dict:
    splits = jax.random.split(jax.random.key(seed), 8)
    hidden_in = scatter_about(splits[0], (TOKENS, D), 1.0, 6.0, ((0, 64),))
    out_grad = scatter_about(splits[1], (TOKENS, D), 1.0, 6.0, ((0, 64),))
    expert_ids_keys = jax.random.split(jax.random.fold_in(splits[2], 1), TOKENS // TOK_DEV)
    expert_ids_turns = jax.random.permutation(jax.random.fold_in(splits[2], 3), TOKENS // TOK_DEV)
    expert_ids = jax.vmap(lambda own, number: shared_out(jax.random.fold_in(splits[2], 2), own, number, TOK_DEV, EXPERTS, TOP, CAP, 2))(expert_ids_keys, expert_ids_turns).reshape((TOKENS, TOP))
    gate_values = jnp.clip(jnp.exp(math.log(1.0) - 2.306499 * jax.random.uniform(splits[3], (TOKENS, TOP), jnp.float32) ** block_scale(splits[3], (TOKENS, TOP), ((0, 64),), -0.2, 0.2)), 0.099609375, 1.0).astype(jnp.bfloat16)
    w_gate = scatter_about(splits[4], (EXPERTS, FF, D), D ** -0.5, 0.09375, ((0, 2), (1, 64)))
    w_up = scatter_about(splits[5], (EXPERTS, FF, D), D ** -0.5, 0.09375, ((0, 2), (1, 64)))
    w_down = scatter_about(splits[6], (EXPERTS, FF, D), FF ** -0.5, 0.046875, ((0, 2), (1, 64)))
    return dict(hidden_in=hidden_in, out_grad=out_grad, expert_ids=expert_ids, gate_values=gate_values, w_gate=w_gate, w_up=w_up, w_down=w_down)


def routed(expert_ids, gate_values, expert, blocks):
    chosen = expert_ids == expert
    hits = jnp.any(chosen, axis=1).astype(jnp.int32).reshape(blocks, TOK_DEV)
    weight = jnp.sum(jnp.where(chosen, gate_values.astype(jnp.float32), jnp.float32(0.0)), axis=1).reshape(blocks, TOK_DEV)
    position = jnp.cumsum(hits, axis=1) - hits
    slot_index = lax.broadcasted_iota(jnp.int32, (blocks, CAP, TOK_DEV), 1)
    picked = (position[:, None, :] == slot_index) & (hits[:, None, :] > 0)
    selector = jnp.where(picked, jnp.float32(1.0), jnp.float32(0.0))
    return selector, weight, chosen


def expert_pass(selector, weight, hidden_in, out_grad, gate_mat, up_mat, down_mat, blocks):
    width = hidden_in.shape[1]
    high = lax.Precision.HIGHEST
    x_slots = jnp.einsum("bct,btd->bcd", selector, hidden_in.reshape(blocks, TOK_DEV, width).astype(jnp.float32), precision=high).astype(jnp.bfloat16).reshape(-1, width)
    dy_slots = jnp.einsum("bct,btd->bcd", selector, out_grad.reshape(blocks, TOK_DEV, width).astype(jnp.float32), precision=high).astype(jnp.bfloat16).reshape(-1, width)
    slot_weight = jnp.einsum("bct,bt->bc", selector, weight, precision=high).reshape(-1, 1)
    gate_pre = jnp.dot(x_slots, gate_mat.T, preferred_element_type=jnp.float32)
    up_pre = jnp.dot(x_slots, up_mat.T, preferred_element_type=jnp.float32)
    back = jnp.dot(dy_slots, down_mat.T, preferred_element_type=jnp.float32)
    sigmoid_gate = jax.nn.sigmoid(gate_pre)
    activation = gate_pre * sigmoid_gate * up_pre
    slot_gate = jnp.sum(activation * back, axis=1)
    dact = slot_weight * back
    d_up = (dact * gate_pre * sigmoid_gate).astype(jnp.bfloat16)
    d_gate = (dact * up_pre * sigmoid_gate * (1.0 + gate_pre * (1.0 - sigmoid_gate))).astype(jnp.bfloat16)
    act_low = activation.astype(jnp.bfloat16)
    dy_weighted = (slot_weight * dy_slots.astype(jnp.float32)).astype(jnp.bfloat16)
    grad_g = jnp.dot(d_gate.T, x_slots, preferred_element_type=jnp.float32).astype(jnp.bfloat16)
    grad_u = jnp.dot(d_up.T, x_slots, preferred_element_type=jnp.float32).astype(jnp.bfloat16)
    grad_d = jnp.dot(act_low.T, dy_weighted, preferred_element_type=jnp.float32).astype(jnp.bfloat16)
    dx_slots = jnp.dot(d_gate, gate_mat, preferred_element_type=jnp.float32) + jnp.dot(d_up, up_mat, preferred_element_type=jnp.float32)
    dx_tokens = jnp.einsum("bct,bcd->btd", selector, dx_slots.reshape(blocks, CAP, width), precision=high).reshape(-1, width)
    gate_tokens = jnp.einsum("bct,bc->bt", selector, slot_gate.reshape(blocks, CAP), precision=high).reshape(-1)
    return grad_g, grad_u, grad_d, dx_tokens, gate_tokens


def reference(hidden_in, out_grad, expert_ids, gate_values, w_gate, w_up, w_down):
    blocks = hidden_in.shape[0] // TOK_DEV
    token_grad = jnp.zeros(hidden_in.shape, jnp.float32)
    gate_grad = jnp.zeros(expert_ids.shape, jnp.float32)
    grads_g, grads_u, grads_d = [], [], []
    for expert in range(w_gate.shape[0]):
        selector, weight, chosen = routed(expert_ids, gate_values, expert, blocks)
        grad_g, grad_u, grad_d, dx_tokens, gate_tokens = expert_pass(selector, weight, hidden_in, out_grad, w_gate[expert], w_up[expert], w_down[expert], blocks)
        grads_g.append(grad_g)
        grads_u.append(grad_u)
        grads_d.append(grad_d)
        token_grad = token_grad + dx_tokens
        gate_grad = gate_grad + jnp.where(chosen, gate_tokens[:, None], jnp.float32(0.0))
    return (token_grad.astype(jnp.bfloat16), gate_grad, jnp.stack(grads_g), jnp.stack(grads_u), jnp.stack(grads_d))
```

```python
import functools

import jax
import jax.numpy as jnp
from jax import lax
from jax.experimental import pallas as pl
from jax.experimental.pallas import tpu as pltpu
from jax.sharding import PartitionSpec as P


AXES = ("blk", "ep")
X, Z, Y, CORE, EP = 4, 4, 2, 2, 2
D = 4096
EXTRA = 128
EXPERTS = 4
TILE = 512
BF16, F32 = jnp.bfloat16, jnp.float32


def place(i):
    i, e = divmod(i, EP)
    i, c = divmod(i, CORE)
    i, y = divmod(i, Y)
    x, z = divmod(i, Z)
    return x, z, y, c, e


def index(x, z, y, c, e):
    return ((((x % X) * Z + z % Z) * Y + y % Y) * CORE + c % CORE) * EP + e % EP


def pairs(to):
    return [(i, index(*to(*place(i)))) for i in range(X * Z * Y * CORE * EP)]


def first(by):
    return pairs(lambda x, z, y, c, e: (x + by * (c == 0), z + by * (c == 1), y, c, e))


def second(by):
    return pairs(lambda x, z, y, c, e: (x + by * (c == 1), z + by * (c == 0), y, c, e))


OTHER_Y = pairs(lambda x, z, y, c, e: (x, z, y + 1, c, e))
OTHER_CORE = pairs(lambda x, z, y, c, e: (x, z, y, c + 1, e))
OTHER_EP = pairs(lambda x, z, y, c, e: (x, z, y, c, e + 1))


def sent(value, to):
    return lax.ppermute(value, AXES, to)


def ring(v, step):
    half = v.shape[0] // 2
    ahead, behind = sent(v, step(-1)), sent(v, step(1))
    far_a = sent(ahead[:half], step(-1))
    return ahead, behind, far_a, sent(behind[half:], step(1))


def plus(a, *others):
    total = a.astype(F32)
    for b in others:
        total = total + b.astype(F32)
    return total.astype(BF16)


def ring_back(own, ahead, behind, far, step):
    half = own.shape[0] // 2
    to_ahead = sent(far[:half], step(1))
    to_behind = sent(far[half:], step(-1))
    ahead = jnp.concatenate([plus(ahead[:half], to_ahead), ahead[half:]], axis=0)
    behind = jnp.concatenate([behind[:half], plus(behind[half:], to_behind)], axis=0)
    up = sent(ahead, step(1))
    return plus(own, up, sent(behind, step(-1)))


NT = (((1,), (1,)), ((), ()))


def expert_kernel(count, held, at, ep_ref, *refs):
    chunks = refs[:count]
    wg_ref, wu_ref, wd_ref = refs[count : count + 3]
    mine_ref, theirs_ref, x_ref, y_ref, coef_ref, cg, cu = refs[count + 3 + held :]
    extra = []
    tokens = cg.shape[0]
    begin = at
    for c in chunks:
        rows = c.shape[0]
        x_ref[at : at + rows, :] = c[:, :D]
        y_ref[at : at + rows, :] = c[:, D : 2 * D]
        extra.append(c[:, 2 * D :].astype(F32))
        at += rows
    xs, ys = x_ref.at[begin:at, :], y_ref.at[begin:at, :]
    coef_ref = coef_ref.at[:, begin:at]
    extra = jnp.concatenate(extra, axis=0).T
    low = ep_ref[0] == 0
    hidden = wg_ref.shape[0] // 2
    gate = lax.dot_general(wg_ref[...], xs[...], NT, preferred_element_type=F32)
    up = lax.dot_general(wu_ref[...], xs[...], NT, preferred_element_type=F32)
    back = lax.dot_general(wd_ref[...], ys[...], NT, preferred_element_type=F32)
    s = 1.0 / (1.0 + jnp.exp(-gate))
    gs = gate * s
    act = gs * up
    product = act * back
    slot_rows = []
    for e in (0, 1):
        mine = slice(e * hidden, (e + 1) * hidden)
        slot_rows.append(jnp.sum(product[mine], axis=0, keepdims=True))
        weight = jnp.where(low, extra[e : e + 1, :], extra[e + 2 : e + 3, :])
        dact = weight * back[mine]
        dgate = dact * up[mine] * s[mine] * (1.0 + gate[mine] * (1.0 - s[mine]))
        coef_ref[e * hidden : (e + 1) * hidden, :] = dgate.astype(BF16)
        coef_ref[(2 + e) * hidden : (3 + e) * hidden, :] = (dact * gs[mine]).astype(BF16)
        coef_ref[(4 + e) * hidden : (5 + e) * hidden, :] = (weight * act[mine]).astype(BF16)
    cg[...] = coef_ref[: 2 * hidden, :].astype(F32).T.astype(BF16)
    cu[...] = coef_ref[2 * hidden : 4 * hidden, :].astype(F32).T.astype(BF16)
    half = tokens // 2

    def column(j, carry):
        cols = pl.ds(pl.multiple_of(j * TILE, TILE), TILE)
        dx = jnp.dot(cg[...], wg_ref[:, cols], preferred_element_type=F32) + jnp.dot(
            cu[...], wu_ref[:, cols], preferred_element_type=F32
        )
        mine_ref[:, cols] = dx[:half].astype(BF16)
        theirs_ref[:, cols] = dx[half:].astype(BF16)
        return carry

    lax.fori_loop(0, D // TILE, column, 0)
    row = lax.broadcasted_iota(jnp.int32, (EXTRA, tokens), 0)
    base = 2 * ep_ref[0]
    slot = jnp.where(row == base, slot_rows[0], 0.0) + jnp.where(row == base + 1, slot_rows[1], 0.0)
    slot = slot.T.astype(BF16)
    mine_ref[:, D:] = slot[:half]
    theirs_ref[:, D:] = slot[half:]


def expert_group(ep, chunks, weights, held, at, total):
    tokens = sum(c.shape[0] for c in chunks)
    hidden2 = weights[0].shape[0]
    vm = pl.BlockSpec(memory_space=pltpu.VMEM)
    part = jax.ShapeDtypeStruct((tokens // 2, D + EXTRA), BF16)
    whole = jax.ShapeDtypeStruct((total, D), BF16)
    before = 1 + len(chunks) + 3
    mine, theirs, *held = pl.pallas_call(
        functools.partial(expert_kernel, len(chunks), len(held), at),
        out_shape=(part, part, whole, whole, jax.ShapeDtypeStruct((3 * hidden2, total), BF16)),
        in_specs=[pl.BlockSpec(memory_space=pltpu.SMEM)] + [vm] * (len(chunks) + 3 + len(held)),
        out_specs=(vm,) * 5,
        scratch_shapes=[pltpu.VMEM((tokens, hidden2), BF16), pltpu.VMEM((tokens, hidden2), BF16)],
        input_output_aliases={before + i: 2 + i for i in range(len(held))},
        cost_estimate=pl.CostEstimate(
            flops=2 * tokens * D * hidden2 * 5,
            bytes_accessed=3 * hidden2 * D * 2 + tokens * 3 * D * 2,
            transcendentals=0,
        ),
        compiler_params=pltpu.CompilerParams(vmem_limit_bytes=8 * 1024 * 1024),
        name="experts",
    )(ep, *chunks, *weights, *held)
    return mine, theirs, held


def weight_kernel(which, side_ref, coef_ref, out_ref):
    h = out_ref.shape[0]
    cols = pl.ds(pl.multiple_of(pl.program_id(0) * TILE, TILE), TILE)
    out_ref[...] = jnp.dot(
        coef_ref[which * h : (which + 1) * h, :], side_ref[:, cols], preferred_element_type=F32
    ).astype(BF16)


def weight_grad(which, side, coef):
    tokens, hidden2 = side.shape[0], coef.shape[0] // 3
    vm = pl.BlockSpec(memory_space=pltpu.VMEM)
    return pl.pallas_call(
        functools.partial(weight_kernel, which),
        grid=(D // TILE,),
        out_shape=jax.ShapeDtypeStruct((hidden2, D), BF16),
        in_specs=[vm, vm],
        out_specs=pl.BlockSpec((hidden2, TILE), lambda j: (0, j)),
        cost_estimate=pl.CostEstimate(
            flops=2 * tokens * D * hidden2,
            bytes_accessed=hidden2 * D * 2 + tokens * D * 2,
            transcendentals=0,
        ),
        compiler_params=pltpu.CompilerParams(vmem_limit_bytes=8 * 1024 * 1024),
        name="weights",
    )(side, coef)


def shards(hidden_in, out_grad, expert_ids, gate_values, w_gate, w_up, w_down):
    local, hidden = w_gate.shape[:2]
    wg, wu, wd = (w.reshape(local * hidden, D) for w in (w_gate, w_up, w_down))
    ep = lax.axis_index("ep").astype(jnp.int32).reshape(1)
    experts = lax.broadcasted_iota(jnp.int32, (1, EXTRA), 1)
    weights = sum(
        jnp.where(expert_ids[:, k : k + 1] == experts, gate_values[:, k : k + 1], 0)
        for k in range(expert_ids.shape[1])
    ).astype(BF16)
    own = jnp.concatenate([hidden_in, out_grad, weights], axis=1)

    two = jnp.concatenate([own, sent(own, OTHER_Y)], axis=0)
    near = jnp.concatenate([two, *ring(two, first)], axis=0)
    near_c = sent(near, OTHER_CORE)
    ahead, behind, far_a, far_b = ring(near, second)
    ahead_c, behind_c = sent(ahead, OTHER_CORE), sent(behind, OTHER_CORE)
    far_ac, far_bc = sent(far_a, OTHER_CORE), sent(far_b, OTHER_CORE)

    groups = ((near, near_c), (ahead, ahead_c), (behind, behind_c), (far_a, far_b, far_ac, far_bc))
    sums, held, at = [], (), 0
    tokens = hidden_in.shape[0] * X * Z * Y * CORE
    for group in groups:
        mine, theirs, held = expert_group(ep, group, (wg, wu, wd), held, at, tokens)
        at += sum(c.shape[0] for c in group)
        sums.append(plus(mine, sent(theirs, OTHER_CORE)))
    x_all, y_all, coef_all = held

    total = ring_back(*sums, second)
    q = total.shape[0] // 4
    total = ring_back(*(total[i * q : (i + 1) * q] for i in range(4)), first)
    q = total.shape[0] // 2
    total = plus(total[:q], sent(total[q:], OTHER_Y))
    other = sent(total, OTHER_EP)
    total = total.astype(F32) + other.astype(F32)
    input_grad = total[:, :D].astype(BF16)
    slot = total[:, D : D + EXPERTS]
    ids = lax.broadcasted_iota(jnp.int32, (1, 1, EXPERTS), 2)
    gate_grad = jnp.sum(jnp.where(expert_ids[:, :, None] == ids, slot[:, None, :], 0.0), axis=2)

    grads = []
    for which, side in enumerate((x_all, x_all, y_all)):
        grads.append(weight_grad(which, side, coef_all).reshape(local, hidden, D))
    return (input_grad, gate_grad, *grads)


def solution(mesh):
    rows, split = P("blk", None), P("ep", "blk", None)
    return jax.shard_map(
        shards,
        mesh=mesh,
        in_specs=(rows, rows, rows, rows, split, split, split),
        out_specs=(rows, rows, split, split, split),
        check_vma=False,
    )
```

```python
import functools

import jax
import jax.numpy as jnp
from jax import lax
from jax.experimental import pallas as pl
from jax.experimental.pallas import tpu as pltpu
from jax.sharding import PartitionSpec as P


AXES = ("blk", "ep")
X, Z, Y, CORE, EP = 4, 4, 2, 2, 2
D = 4096
EXTRA = 128
EXPERTS = 4
TILE = 1024
BF16, F32 = jnp.bfloat16, jnp.float32


def place(i):
    i, e = divmod(i, EP)
    i, c = divmod(i, CORE)
    i, y = divmod(i, Y)
    x, z = divmod(i, Z)
    return x, z, y, c, e


def index(x, z, y, c, e):
    return ((((x % X) * Z + z % Z) * Y + y % Y) * CORE + c % CORE) * EP + e % EP


def pairs(to):
    return [(i, index(*to(*place(i)))) for i in range(X * Z * Y * CORE * EP)]


def first(by):
    return pairs(lambda x, z, y, c, e: (x + by * (c == 0), z + by * (c == 1), y, c, e))


def second(by):
    return pairs(lambda x, z, y, c, e: (x + by * (c == 1), z + by * (c == 0), y, c, e))


OTHER_Y = pairs(lambda x, z, y, c, e: (x, z, y + 1, c, e))
OTHER_CORE = pairs(lambda x, z, y, c, e: (x, z, y, c + 1, e))
OTHER_EP = pairs(lambda x, z, y, c, e: (x, z, y, c, e + 1))
OTHER_BOTH = pairs(lambda x, z, y, c, e: (x, z, y + 1, c, e + 1))


def sent(value, to):
    return lax.ppermute(value, AXES, to)


def joined_kernel(*refs):
    out, at = refs[-1], 0
    for r in refs[:-1]:
        out[at : at + r.shape[0], :] = r[...]
        at += r.shape[0]


def packed_kernel(ep_ref, x_ref, y_ref, extra_ref, out_ref, done):
    wide = x_ref.shape[1]
    x_copy = pltpu.make_async_copy(x_ref, out_ref.at[:, :wide], done.at[0])
    y_copy = pltpu.make_async_copy(y_ref, out_ref.at[:, wide : 2 * wide], done.at[1])
    x_copy.start()
    y_copy.start()
    out_ref[:, 2 * wide :] = extra_ref[...]
    x_copy.wait()
    y_copy.wait()


VM = pl.BlockSpec(memory_space=pltpu.VMEM)


def joined(*arrays):
    shape = (sum(a.shape[0] for a in arrays), arrays[0].shape[1])
    return pl.pallas_call(
        joined_kernel,
        out_shape=jax.ShapeDtypeStruct(shape, BF16),
        in_specs=[VM] * len(arrays),
        out_specs=VM,
        compiler_params=pltpu.CompilerParams(vmem_limit_bytes=8 * 1024 * 1024),
        name="joined",
    )(*arrays)


def taken_kernel(start, v_ref, out_ref):
    out_ref[...] = v_ref[start : start + out_ref.shape[0], :]


def taken(v, start, rows):
    return pl.pallas_call(
        functools.partial(taken_kernel, start),
        out_shape=jax.ShapeDtypeStruct((rows, v.shape[1]), BF16),
        in_specs=[VM],
        out_specs=VM,
        compiler_params=pltpu.CompilerParams(vmem_limit_bytes=8 * 1024 * 1024),
        name="taken",
    )(v)


def packed(ep, x, y, extra):
    shape = (x.shape[0], x.shape[1] + y.shape[1] + extra.shape[1])
    held = pl.BlockSpec(memory_space=pltpu.HBM)
    return pl.pallas_call(
        packed_kernel,
        out_shape=jax.ShapeDtypeStruct(shape, BF16),
        in_specs=[pl.BlockSpec(memory_space=pltpu.SMEM), held, held, VM],
        out_specs=VM,
        scratch_shapes=[pltpu.SemaphoreType.DMA((2,))],
        compiler_params=pltpu.CompilerParams(vmem_limit_bytes=60 * 1024 * 1024),
        name="packed",
    )(ep, x, y, extra)


def touched_kernel(*refs):
    refs[-1][...] = jnp.zeros_like(refs[-1])


def touched(*arrays):
    return pl.pallas_call(
        touched_kernel,
        out_shape=jax.ShapeDtypeStruct((8, 128), F32),
        in_specs=[VM] * len(arrays),
        out_specs=VM,
        compiler_params=pltpu.CompilerParams(
            vmem_limit_bytes=1024 * 1024, has_side_effects=True
        ),
        name="touched",
    )(*arrays)


STEP = 16


def sums_kernel(plan, count, *refs):
    ins, outs = refs[:count], refs[count:]
    for out, (rows, terms) in zip(outs, plan):
        for r in range(0, rows, STEP):
            total = None
            for i, source, first_row, n in terms:
                if first_row <= r < first_row + n:
                    at = source + r - first_row
                    part = ins[i][at : at + STEP, :].astype(F32)
                    total = part if total is None else total + part
            out[r : r + STEP, :] = total.astype(BF16)


def sums(arrays, plan):
    width = arrays[0].shape[1]
    return pl.pallas_call(
        functools.partial(sums_kernel, plan, len(arrays)),
        out_shape=tuple(jax.ShapeDtypeStruct((rows, width), BF16) for rows, _ in plan),
        in_specs=[VM] * len(arrays),
        out_specs=(VM,) * len(plan),
        compiler_params=pltpu.CompilerParams(vmem_limit_bytes=8 * 1024 * 1024),
        name="sums",
    )(*arrays)


def last_kernel(own, same, other, other_pair, grad_ref, slot_ref):
    total = (own[...].astype(F32) + same[...].astype(F32)) + (
        other[...].astype(F32) + other_pair[...].astype(F32)
    )
    grad_ref[...] = total[:, :D].astype(BF16)
    slot_ref[...] = total[:, D:]


def last(*arrays):
    rows = arrays[0].shape[0]
    return pl.pallas_call(
        last_kernel,
        out_shape=(
            jax.ShapeDtypeStruct((rows, D), BF16),
            jax.ShapeDtypeStruct((rows, EXTRA), F32),
        ),
        in_specs=[VM] * 4,
        out_specs=(VM, VM),
        compiler_params=pltpu.CompilerParams(vmem_limit_bytes=4 * 1024 * 1024),
        name="last",
    )(*arrays)


NT = (((1,), (1,)), ((), ()))


def expert_kernel(count, held, at, ep_ref, *refs):
    chunks = refs[:count]
    wg_ref, wu_ref, wd_ref = refs[count : count + 3]
    mine_ref, theirs_ref, x_ref, y_ref, coef_ref, cg, cu = refs[count + 3 + held :]
    extra = []
    tokens = cg.shape[0]
    begin = at
    for c in chunks:
        rows = c.shape[0]
        x_ref[at : at + rows, :] = c[:, :D]
        y_ref[at : at + rows, :] = c[:, D : 2 * D]
        extra.append(c[:, 2 * D :].astype(F32))
        at += rows
    xs, ys = x_ref.at[begin:at, :], y_ref.at[begin:at, :]
    coef_ref = coef_ref.at[:, begin:at]
    extra = jnp.concatenate(extra, axis=0).T
    low = ep_ref[0] == 0
    hidden = wg_ref.shape[0] // 2
    gate = lax.dot_general(wg_ref[...], xs[...], NT, preferred_element_type=F32)
    up = lax.dot_general(wu_ref[...], xs[...], NT, preferred_element_type=F32)
    back = lax.dot_general(wd_ref[...], ys[...], NT, preferred_element_type=F32)
    s = 1.0 / (1.0 + jnp.exp(-gate))
    gs = gate * s
    act = gs * up
    product = act * back
    slot_rows = []
    for e in (0, 1):
        mine = slice(e * hidden, (e + 1) * hidden)
        slot_rows.append(jnp.sum(product[mine], axis=0, keepdims=True))
        weight = jnp.where(low, extra[e : e + 1, :], extra[e + 2 : e + 3, :])
        dact = weight * back[mine]
        dgate = dact * up[mine] * s[mine] * (1.0 + gate[mine] * (1.0 - s[mine]))
        coef_ref[e * hidden : (e + 1) * hidden, :] = dgate.astype(BF16)
        coef_ref[(2 + e) * hidden : (3 + e) * hidden, :] = (dact * gs[mine]).astype(BF16)
        coef_ref[(4 + e) * hidden : (5 + e) * hidden, :] = (weight * act[mine]).astype(BF16)
    cg[...] = coef_ref[: 2 * hidden, :].astype(F32).T.astype(BF16)
    cu[...] = coef_ref[2 * hidden : 4 * hidden, :].astype(F32).T.astype(BF16)
    half = tokens // 2

    def column(j, carry):
        cols = pl.ds(pl.multiple_of(j * TILE, TILE), TILE)
        dx = jnp.dot(cg[...], wg_ref[:, cols], preferred_element_type=F32) + jnp.dot(
            cu[...], wu_ref[:, cols], preferred_element_type=F32
        )
        mine_ref[:, cols] = dx[:half].astype(BF16)
        theirs_ref[:, cols] = dx[half:].astype(BF16)
        return carry

    lax.fori_loop(0, D // TILE, column, 0)
    row = lax.broadcasted_iota(jnp.int32, (EXTRA, tokens), 0)
    base = 2 * ep_ref[0]
    slot = jnp.where(row == base, slot_rows[0], 0.0) + jnp.where(row == base + 1, slot_rows[1], 0.0)
    slot = slot.T.astype(BF16)
    mine_ref[:, D:] = slot[:half]
    theirs_ref[:, D:] = slot[half:]


def expert_group(ep, chunks, weights, held, at, total):
    tokens = sum(c.shape[0] for c in chunks)
    hidden2 = weights[0].shape[0]
    part = jax.ShapeDtypeStruct((tokens // 2, D + EXTRA), BF16)
    whole = jax.ShapeDtypeStruct((total, D), BF16)
    before = 1 + len(chunks) + 3
    mine, theirs, *held = pl.pallas_call(
        functools.partial(expert_kernel, len(chunks), len(held), at),
        out_shape=(part, part, whole, whole, jax.ShapeDtypeStruct((3 * hidden2, total), BF16)),
        in_specs=[pl.BlockSpec(memory_space=pltpu.SMEM)] + [VM] * (len(chunks) + 3 + len(held)),
        out_specs=(VM,) * 5,
        scratch_shapes=[pltpu.VMEM((tokens, hidden2), BF16), pltpu.VMEM((tokens, hidden2), BF16)],
        input_output_aliases={before + i: 2 + i for i in range(len(held))},
        cost_estimate=pl.CostEstimate(
            flops=2 * tokens * D * hidden2 * 5,
            bytes_accessed=3 * hidden2 * D * 2 + tokens * 3 * D * 2,
            transcendentals=0,
        ),
        compiler_params=pltpu.CompilerParams(vmem_limit_bytes=8 * 1024 * 1024),
        name="experts",
    )(ep, *chunks, *weights, *held)
    return mine, theirs, held


def weight_kernel(which, side_ref, coef_ref, out_ref):
    h = out_ref.shape[0]
    cols = pl.ds(pl.multiple_of(pl.program_id(0) * TILE, TILE), TILE)
    out_ref[...] = jnp.dot(
        coef_ref[which * h : (which + 1) * h, :], side_ref[:, cols], preferred_element_type=F32
    ).astype(BF16)


def weight_grad(which, side, coef):
    tokens, hidden2 = side.shape[0], coef.shape[0] // 3
    return pl.pallas_call(
        functools.partial(weight_kernel, which),
        grid=(D // TILE,),
        out_shape=jax.ShapeDtypeStruct((hidden2, D), BF16),
        in_specs=[VM, VM],
        out_specs=pl.BlockSpec((hidden2, TILE), lambda j: (0, j)),
        cost_estimate=pl.CostEstimate(
            flops=2 * tokens * D * hidden2,
            bytes_accessed=hidden2 * D * 2 + tokens * D * 2,
            transcendentals=0,
        ),
        compiler_params=pltpu.CompilerParams(vmem_limit_bytes=8 * 1024 * 1024),
        name="weights",
    )(side, coef)


def shards(hidden_in, out_grad, expert_ids, gate_values, w_gate, w_up, w_down):
    local, hidden = w_gate.shape[:2]
    wg, wu, wd = (w.reshape(local * hidden, D) for w in (w_gate, w_up, w_down))
    touched(wg, wu, wd)
    ep = lax.axis_index("ep").astype(jnp.int32).reshape(1)
    experts = lax.broadcasted_iota(jnp.int32, (1, 1, EXTRA), 2)
    chosen = expert_ids[:, :, None] == experts
    weights = jnp.sum(jnp.where(chosen, gate_values[:, :, None], jnp.zeros((), BF16)), axis=1)
    own = packed(ep, hidden_in, out_grad, weights)
    one = own.shape[0]
    two = joined(own, sent(own, OTHER_Y))

    n_a, n_b = sent(two, first(-1)), sent(two, first(1))
    n_far = sent(two, first(2))
    near = joined(n_a, n_b)
    m_a, m_b = sent(near, second(-1)), sent(near, second(1))
    rest = joined(two, n_far)
    e_a, e_b = sent(rest, second(-1)), sent(rest, second(1))
    h = two.shape[0]
    fm_a = sent(taken(m_a, 0, h), second(-1))
    fm_b = sent(taken(m_b, h, h), second(1))
    fe_a = sent(taken(e_a, 0, h), second(-1))
    fe_b = sent(taken(e_b, h, h), second(1))

    groups = []
    for group in ((near, rest), (m_a, m_b), (e_a, e_b), (fm_a, fm_b, fe_a, fe_b)):
        both = [sent(c, OTHER_CORE) for c in group]
        groups.append((*group, *both))

    parts, held, at = {}, (), 0
    tokens = one * X * Z * Y * CORE
    for g in (0, 1, 3, 2):
        group = groups[g]
        mine, theirs, held = expert_group(ep, group, (wg, wu, wd), held, at, tokens)
        at += sum(c.shape[0] for c in group)
        parts[g] = (mine, sent(theirs, OTHER_CORE))
    x_all, y_all, coef_all = held

    up, down = sums(
        parts[3],
        tuple(
            (2 * h, tuple((i, s * h + k * 2 * h, k * h, h) for i in (0, 1) for k in (0, 1)))
            for s in (0, 1)
        ),
    )
    up, down = sent(up, second(1)), sent(down, second(-1))
    n = 2 * h
    g_a, t_a, g_b, t_b = sums(
        (*parts[1], up, *parts[2], down),
        (
            (3 * h, ((0, 0, 0, n), (1, 0, 0, n), (2, 0, 0, h), (3, h, n, h), (4, h, n, h))),
            (h, ((3, 0, 0, h), (4, 0, 0, h), (2, h, 0, h))),
            (
                3 * h,
                ((0, n, 0, n), (1, n, 0, n), (5, 0, h, h))
                + ((3, n + h, n, h), (4, n + h, n, h), (5, h, n, h)),
            ),
            (h, ((3, n, 0, h), (4, n, 0, h))),
        ),
    )
    g_a, g_b = sent(g_a, second(1)), sent(g_b, second(-1))
    t_a, t_b = sent(t_a, second(1)), sent(t_b, second(-1))
    n_a, n_b, n_far = sums(
        (*parts[0], g_a, g_b),
        tuple(
            (h, ((0, at, 0, h), (1, at, 0, h), (2, i * h, 0, h), (3, i * h, 0, h)))
            for i, at in enumerate((0, h, 3 * h))
        ),
    )
    n_a, n_b = sent(n_a, first(1)), sent(n_b, first(-1))
    n_far = sent(n_far, first(2))
    own, pair = sums(
        (*parts[0], t_a, t_b, n_a, n_b, n_far),
        tuple(
            (one, tuple((i, a * one + (n if i < 2 else 0), 0, one) for i in range(7)))
            for a in range(2)
        ),
    )
    same = sent(pair, OTHER_Y)
    other, other_pair = sent(own, OTHER_EP), sent(pair, OTHER_BOTH)
    input_grad, slot = last(own, same, other, other_pair)
    picked = expert_ids[:, :, None] == lax.broadcasted_iota(jnp.int32, (1, 1, EXPERTS), 2)
    gate_grad = jnp.sum(jnp.where(picked, slot[:, None, :EXPERTS], 0.0), axis=2)

    grads = []
    for which, side in enumerate((x_all, x_all, y_all)):
        grads.append(weight_grad(which, side, coef_all).reshape(local, hidden, D))
    return (input_grad, gate_grad, *grads)


def solution(mesh):
    rows, split = P("blk", None), P("ep", "blk", None)
    return jax.shard_map(
        shards,
        mesh=mesh,
        in_specs=(rows, rows, rows, rows, split, split, split),
        out_specs=(rows, rows, split, split, split),
        check_vma=False,
    )
```

```python
import functools

import jax
import jax.numpy as jnp
from jax import lax
from jax.experimental import pallas as pl
from jax.experimental.pallas import tpu as pltpu
from jax.sharding import PartitionSpec as P


AXES = ("blk", "ep")
X, Z, Y, CORE, EP = 4, 4, 2, 2, 2
D = 4096
EXTRA = 128
EXPERTS = 4
TILE = 1024
BF16, F32 = jnp.bfloat16, jnp.float32


def place(i):
    i, e = divmod(i, EP)
    i, c = divmod(i, CORE)
    i, y = divmod(i, Y)
    x, z = divmod(i, Z)
    return x, z, y, c, e


def index(x, z, y, c, e):
    return ((((x % X) * Z + z % Z) * Y + y % Y) * CORE + c % CORE) * EP + e % EP


def pairs(to):
    return [(i, index(*to(*place(i)))) for i in range(X * Z * Y * CORE * EP)]


def first(by):
    return pairs(lambda x, z, y, c, e: (x + by * (c == 0), z + by * (c == 1), y, c, e))


def second(by):
    return pairs(lambda x, z, y, c, e: (x + by * (c == 1), z + by * (c == 0), y, c, e))


OTHER_Y = pairs(lambda x, z, y, c, e: (x, z, y + 1, c, e))
OTHER_CORE = pairs(lambda x, z, y, c, e: (x, z, y, c + 1, e))
OTHER_EP = pairs(lambda x, z, y, c, e: (x, z, y, c, e + 1))
OTHER_BOTH = pairs(lambda x, z, y, c, e: (x, z, y + 1, c, e + 1))


def sent(value, to):
    return lax.ppermute(value, AXES, to)


def joined_kernel(*refs):
    out, at = refs[-1], 0
    for r in refs[:-1]:
        out[at : at + r.shape[0], :] = r[...]
        at += r.shape[0]


def packed_kernel(ep_ref, x_ref, y_ref, extra_ref, out_ref, done):
    wide = x_ref.shape[1]
    x_copy = pltpu.make_async_copy(x_ref, out_ref.at[:, :wide], done.at[0])
    y_copy = pltpu.make_async_copy(y_ref, out_ref.at[:, wide : 2 * wide], done.at[1])
    x_copy.start()
    y_copy.start()
    out_ref[:, 2 * wide :] = extra_ref[...]
    x_copy.wait()
    y_copy.wait()


VM = pl.BlockSpec(memory_space=pltpu.VMEM)


def joined(*arrays):
    shape = (sum(a.shape[0] for a in arrays), arrays[0].shape[1])
    return pl.pallas_call(
        joined_kernel,
        out_shape=jax.ShapeDtypeStruct(shape, BF16),
        in_specs=[VM] * len(arrays),
        out_specs=VM,
        compiler_params=pltpu.CompilerParams(vmem_limit_bytes=8 * 1024 * 1024),
        name="joined",
    )(*arrays)


def taken_kernel(start, v_ref, out_ref):
    out_ref[...] = v_ref[start : start + out_ref.shape[0], :]


def taken(v, start, rows):
    return pl.pallas_call(
        functools.partial(taken_kernel, start),
        out_shape=jax.ShapeDtypeStruct((rows, v.shape[1]), BF16),
        in_specs=[VM],
        out_specs=VM,
        compiler_params=pltpu.CompilerParams(vmem_limit_bytes=8 * 1024 * 1024),
        name="taken",
    )(v)


def packed(ep, x, y, extra):
    shape = (x.shape[0], x.shape[1] + y.shape[1] + extra.shape[1])
    held = pl.BlockSpec(memory_space=pltpu.HBM)
    return pl.pallas_call(
        packed_kernel,
        out_shape=jax.ShapeDtypeStruct(shape, BF16),
        in_specs=[pl.BlockSpec(memory_space=pltpu.SMEM), held, held, VM],
        out_specs=VM,
        scratch_shapes=[pltpu.SemaphoreType.DMA((2,))],
        compiler_params=pltpu.CompilerParams(vmem_limit_bytes=8 * 1024 * 1024),
        name="packed",
    )(ep, x, y, extra)


def touched_kernel(*refs):
    refs[-1][...] = jnp.zeros_like(refs[-1])


def touched(*arrays):
    return pl.pallas_call(
        touched_kernel,
        out_shape=jax.ShapeDtypeStruct((8, 128), F32),
        in_specs=[VM] * len(arrays),
        out_specs=VM,
        compiler_params=pltpu.CompilerParams(
            vmem_limit_bytes=1024 * 1024, has_side_effects=True
        ),
        name="touched",
    )(*arrays)


STEP = 16


def sums_kernel(plan, count, *refs):
    ins, outs = refs[:count], refs[count:]
    for out, (rows, terms) in zip(outs, plan):
        for r in range(0, rows, STEP):
            total = None
            for i, source, first_row, n in terms:
                if first_row <= r < first_row + n:
                    at = source + r - first_row
                    part = ins[i][at : at + STEP, :].astype(F32)
                    total = part if total is None else total + part
            out[r : r + STEP, :] = total.astype(BF16)


def sums(arrays, plan):
    width = arrays[0].shape[1]
    return pl.pallas_call(
        functools.partial(sums_kernel, plan, len(arrays)),
        out_shape=tuple(jax.ShapeDtypeStruct((rows, width), BF16) for rows, _ in plan),
        in_specs=[VM] * len(arrays),
        out_specs=(VM,) * len(plan),
        compiler_params=pltpu.CompilerParams(vmem_limit_bytes=8 * 1024 * 1024),
        name="sums",
    )(*arrays)


def last_kernel(own, same, other, other_pair, grad_ref, slot_ref):
    total = (own[...].astype(F32) + same[...].astype(F32)) + (
        other[...].astype(F32) + other_pair[...].astype(F32)
    )
    grad_ref[...] = total[:, :D].astype(BF16)
    slot_ref[...] = total[:, D:]


def last(*arrays):
    rows = arrays[0].shape[0]
    return pl.pallas_call(
        last_kernel,
        out_shape=(
            jax.ShapeDtypeStruct((rows, D), BF16),
            jax.ShapeDtypeStruct((rows, EXTRA), F32),
        ),
        in_specs=[VM] * 4,
        out_specs=(VM, VM),
        compiler_params=pltpu.CompilerParams(vmem_limit_bytes=4 * 1024 * 1024),
        name="last",
    )(*arrays)


NT = (((1,), (1,)), ((), ()))


def expert_kernel(count, held, at, ep_ref, *refs):
    chunks = refs[:count]
    wg_ref, wu_ref, wd_ref = refs[count : count + 3]
    mine_ref, theirs_ref, x_ref, y_ref, coef_ref, cg, cu = refs[count + 3 + held :]
    extra = []
    tokens = cg.shape[0]
    begin = at
    for c in chunks:
        rows = c.shape[0]
        x_ref[at : at + rows, :] = c[:, :D]
        y_ref[at : at + rows, :] = c[:, D : 2 * D]
        extra.append(c[:, 2 * D :].astype(F32))
        at += rows
    xs, ys = x_ref.at[begin:at, :], y_ref.at[begin:at, :]
    coef_ref = coef_ref.at[:, begin:at]
    extra = jnp.concatenate(extra, axis=0).T
    low = ep_ref[0] == 0
    hidden = wg_ref.shape[0] // 2
    gate = lax.dot_general(wg_ref[...], xs[...], NT, preferred_element_type=F32)
    up = lax.dot_general(wu_ref[...], xs[...], NT, preferred_element_type=F32)
    back = lax.dot_general(wd_ref[...], ys[...], NT, preferred_element_type=F32)
    s = 1.0 / (1.0 + jnp.exp(-gate))
    gs = gate * s
    act = gs * up
    product = act * back
    slot_rows = []
    for e in (0, 1):
        mine = slice(e * hidden, (e + 1) * hidden)
        slot_rows.append(jnp.sum(product[mine], axis=0, keepdims=True))
        weight = jnp.where(low, extra[e : e + 1, :], extra[e + 2 : e + 3, :])
        dact = weight * back[mine]
        dgate = dact * up[mine] * s[mine] * (1.0 + gate[mine] * (1.0 - s[mine]))
        coef_ref[e * hidden : (e + 1) * hidden, :] = dgate.astype(BF16)
        coef_ref[(2 + e) * hidden : (3 + e) * hidden, :] = (dact * gs[mine]).astype(BF16)
        coef_ref[(4 + e) * hidden : (5 + e) * hidden, :] = (weight * act[mine]).astype(BF16)
    cg[...] = coef_ref[: 2 * hidden, :].astype(F32).T.astype(BF16)
    cu[...] = coef_ref[2 * hidden : 4 * hidden, :].astype(F32).T.astype(BF16)
    half = tokens // 2

    def column(j, carry):
        cols = pl.ds(pl.multiple_of(j * TILE, TILE), TILE)
        dx = jnp.dot(cg[...], wg_ref[:, cols], preferred_element_type=F32) + jnp.dot(
            cu[...], wu_ref[:, cols], preferred_element_type=F32
        )
        mine_ref[:, cols] = dx[:half].astype(BF16)
        theirs_ref[:, cols] = dx[half:].astype(BF16)
        return carry

    lax.fori_loop(0, D // TILE, column, 0)
    row = lax.broadcasted_iota(jnp.int32, (EXTRA, tokens), 0)
    base = 2 * ep_ref[0]
    slot = jnp.where(row == base, slot_rows[0], 0.0) + jnp.where(row == base + 1, slot_rows[1], 0.0)
    slot = slot.T.astype(BF16)
    mine_ref[:, D:] = slot[:half]
    theirs_ref[:, D:] = slot[half:]


def expert_group(ep, chunks, weights, held, at, total):
    tokens = sum(c.shape[0] for c in chunks)
    hidden2 = weights[0].shape[0]
    part = jax.ShapeDtypeStruct((tokens // 2, D + EXTRA), BF16)
    whole = jax.ShapeDtypeStruct((total, D), BF16)
    before = 1 + len(chunks) + 3
    mine, theirs, *held = pl.pallas_call(
        functools.partial(expert_kernel, len(chunks), len(held), at),
        out_shape=(part, part, whole, whole, jax.ShapeDtypeStruct((3 * hidden2, total), BF16)),
        in_specs=[pl.BlockSpec(memory_space=pltpu.SMEM)] + [VM] * (len(chunks) + 3 + len(held)),
        out_specs=(VM,) * 5,
        scratch_shapes=[pltpu.VMEM((tokens, hidden2), BF16), pltpu.VMEM((tokens, hidden2), BF16)],
        input_output_aliases={before + i: 2 + i for i in range(len(held))},
        cost_estimate=pl.CostEstimate(
            flops=2 * tokens * D * hidden2 * 5,
            bytes_accessed=3 * hidden2 * D * 2 + tokens * 3 * D * 2,
            transcendentals=0,
        ),
        compiler_params=pltpu.CompilerParams(vmem_limit_bytes=8 * 1024 * 1024),
        name="experts",
    )(ep, *chunks, *weights, *held)
    return mine, theirs, held


def weight_kernel(which, side_ref, coef_ref, out_ref):
    h = out_ref.shape[0]
    cols = pl.ds(pl.multiple_of(pl.program_id(0) * TILE, TILE), TILE)
    out_ref[...] = jnp.dot(
        coef_ref[which * h : (which + 1) * h, :], side_ref[:, cols], preferred_element_type=F32
    ).astype(BF16)


def weight_grad(which, side, coef):
    tokens, hidden2 = side.shape[0], coef.shape[0] // 3
    return pl.pallas_call(
        functools.partial(weight_kernel, which),
        grid=(D // TILE,),
        out_shape=jax.ShapeDtypeStruct((hidden2, D), BF16),
        in_specs=[VM, VM],
        out_specs=pl.BlockSpec((hidden2, TILE), lambda j: (0, j)),
        cost_estimate=pl.CostEstimate(
            flops=2 * tokens * D * hidden2,
            bytes_accessed=hidden2 * D * 2 + tokens * D * 2,
            transcendentals=0,
        ),
        compiler_params=pltpu.CompilerParams(vmem_limit_bytes=8 * 1024 * 1024),
        name="weights",
    )(side, coef)


def shards(hidden_in, out_grad, expert_ids, gate_values, w_gate, w_up, w_down):
    local, hidden = w_gate.shape[:2]
    wg, wu, wd = (w.reshape(local * hidden, D) for w in (w_gate, w_up, w_down))
    touched(wg, wu, wd)
    ep = lax.axis_index("ep").astype(jnp.int32).reshape(1)
    experts = lax.broadcasted_iota(jnp.int32, (1, 1, EXTRA), 2)
    chosen = expert_ids[:, :, None] == experts
    weights = jnp.sum(jnp.where(chosen, gate_values[:, :, None], jnp.zeros((), BF16)), axis=1)
    own = packed(ep, hidden_in, out_grad, weights)
    one = own.shape[0]
    two = joined(own, sent(own, OTHER_Y))

    n_a, n_b, n_far = sent(two, first(-1)), sent(two, first(1)), sent(two, first(2))
    near = joined(n_a, n_b, two)
    m_a, m_b = sent(near, second(-1)), sent(near, second(1))
    e_a, e_b = sent(n_far, second(-1)), sent(n_far, second(1))
    k, j = near.shape[0] // 2, n_far.shape[0] // 2
    fm_a, fm_b = sent(taken(m_a, 0, k), second(-1)), sent(taken(m_b, k, k), second(1))
    fe_a, fe_b = sent(taken(e_a, 0, j), second(-1)), sent(taken(e_b, j, j), second(1))

    groups = []
    for group in ((near, n_far), (m_a, e_a), (m_b, e_b), (fm_a, fe_a, fm_b, fe_b)):
        both = [sent(c, OTHER_CORE) for c in group]
        groups.append((*group, *both))

    parts, held, at = {}, (), 0
    tokens = one * X * Z * Y * CORE
    for g in (0, 1, 3, 2):
        group = groups[g]
        mine, theirs, held = expert_group(ep, group, (wg, wu, wd), held, at, tokens)
        at += sum(c.shape[0] for c in group)
        parts[g] = (mine, sent(theirs, OTHER_CORE))
    x_all, y_all, coef_all = held

    h, r = two.shape[0], k + j
    n = 2 * h
    up, down = sums(
        parts[3], tuple((r, ((0, i * r, 0, r), (1, i * r, 0, r))) for i in (0, 1))
    )
    up, down = sent(up, second(1)), sent(down, second(-1))
    line = ((0, 0, 0, n), (1, 0, 0, n), (0, n + h, n, h), (1, n + h, n, h))
    g_a, t_a = sums(
        (*parts[1], up),
        (
            (n + h, (*line, (2, 0, 0, k), (2, k, n, j))),
            (h, ((0, n, 0, h), (1, n, 0, h))),
        ),
    )
    g_b, t_b = sums(
        (*parts[2], down),
        (
            (n + h, (*line, (2, 0, k, n - k), (2, k, n + j, j))),
            (h, ((0, n, 0, h), (1, n, 0, h), (2, n - k, 0, h))),
        ),
    )
    g_a, g_b = sent(g_a, second(1)), sent(g_b, second(-1))
    t_a, t_b = sent(t_a, second(1)), sent(t_b, second(-1))
    n_a, n_b, n_far = sums(
        (*parts[0], g_a, g_b),
        tuple(
            (h, ((0, at, 0, h), (1, at, 0, h), (2, i * h, 0, h), (3, i * h, 0, h)))
            for i, at in enumerate((0, h, 3 * h))
        ),
    )
    n_a, n_b = sent(n_a, first(1)), sent(n_b, first(-1))
    n_far = sent(n_far, first(2))
    own, pair = sums(
        (*parts[0], t_a, t_b, n_a, n_b, n_far),
        tuple(
            (one, tuple((i, a * one + (n if i < 2 else 0), 0, one) for i in range(7)))
            for a in range(2)
        ),
    )
    same = sent(pair, OTHER_Y)
    other, other_pair = sent(own, OTHER_EP), sent(pair, OTHER_BOTH)
    input_grad, slot = last(own, same, other, other_pair)
    picked = expert_ids[:, :, None] == lax.broadcasted_iota(jnp.int32, (1, 1, EXPERTS), 2)
    gate_grad = jnp.sum(jnp.where(picked, slot[:, None, :EXPERTS], 0.0), axis=2)

    grads = []
    for which, side in enumerate((x_all, x_all, y_all)):
        grads.append(weight_grad(which, side, coef_all).reshape(local, hidden, D))
    return (input_grad, gate_grad, *grads)


def solution(mesh):
    rows, split = P("blk", None), P("ep", "blk", None)
    return jax.shard_map(
        shards,
        mesh=mesh,
        in_specs=(rows, rows, rows, rows, split, split, split),
        out_specs=(rows, rows, split, split, split),
        check_vma=False,
    )
```

```python
import functools

import jax
import jax.numpy as jnp
from jax import lax
from jax.experimental import pallas as pl
from jax.experimental.pallas import tpu as pltpu
from jax.sharding import PartitionSpec as P


AXES = ("blk", "ep")
X, Z, Y, CORE, EP = 4, 4, 2, 2, 2
D = 4096
EXTRA = 128
EXPERTS = 4
TILE = 1024
BF16, F32 = jnp.bfloat16, jnp.float32


def place(i):
    i, e = divmod(i, EP)
    i, c = divmod(i, CORE)
    i, y = divmod(i, Y)
    x, z = divmod(i, Z)
    return x, z, y, c, e


def index(x, z, y, c, e):
    return ((((x % X) * Z + z % Z) * Y + y % Y) * CORE + c % CORE) * EP + e % EP


def pairs(to):
    return [(i, index(*to(*place(i)))) for i in range(X * Z * Y * CORE * EP)]


def first(by):
    return pairs(lambda x, z, y, c, e: (x + by * (c == 0), z + by * (c == 1), y, c, e))


def second(by):
    return pairs(lambda x, z, y, c, e: (x + by * (c == 1), z + by * (c == 0), y, c, e))


OTHER_Y = pairs(lambda x, z, y, c, e: (x, z, y + 1, c, e))
OTHER_CORE = pairs(lambda x, z, y, c, e: (x, z, y, c + 1, e))
OTHER_EP = pairs(lambda x, z, y, c, e: (x, z, y, c, e + 1))
OTHER_BOTH = pairs(lambda x, z, y, c, e: (x, z, y + 1, c, e + 1))


def sent(value, to):
    return lax.ppermute(value, AXES, to)


def joined_kernel(*refs):
    out, at = refs[-1], 0
    for r in refs[:-1]:
        out[at : at + r.shape[0], :] = r[...]
        at += r.shape[0]


def packed_kernel(ep_ref, x_ref, y_ref, extra_ref, out_ref, done):
    wide = x_ref.shape[1]
    x_copy = pltpu.make_async_copy(x_ref, out_ref.at[:, :wide], done.at[0])
    y_copy = pltpu.make_async_copy(y_ref, out_ref.at[:, wide : 2 * wide], done.at[1])
    x_copy.start()
    y_copy.start()
    out_ref[:, 2 * wide :] = extra_ref[...]
    x_copy.wait()
    y_copy.wait()


VM = pl.BlockSpec(memory_space=pltpu.VMEM)


def joined(*arrays):
    shape = (sum(a.shape[0] for a in arrays), arrays[0].shape[1])
    return pl.pallas_call(
        joined_kernel,
        out_shape=jax.ShapeDtypeStruct(shape, BF16),
        in_specs=[VM] * len(arrays),
        out_specs=VM,
        compiler_params=pltpu.CompilerParams(vmem_limit_bytes=8 * 1024 * 1024),
        name="joined",
    )(*arrays)


def taken_kernel(start, v_ref, out_ref):
    out_ref[...] = v_ref[start : start + out_ref.shape[0], :]


def taken(v, start, rows):
    return pl.pallas_call(
        functools.partial(taken_kernel, start),
        out_shape=jax.ShapeDtypeStruct((rows, v.shape[1]), BF16),
        in_specs=[VM],
        out_specs=VM,
        compiler_params=pltpu.CompilerParams(vmem_limit_bytes=8 * 1024 * 1024),
        name="taken",
    )(v)


def packed(ep, x, y, extra):
    shape = (x.shape[0], x.shape[1] + y.shape[1] + extra.shape[1])
    held = pl.BlockSpec(memory_space=pltpu.HBM)
    return pl.pallas_call(
        packed_kernel,
        out_shape=jax.ShapeDtypeStruct(shape, BF16),
        in_specs=[pl.BlockSpec(memory_space=pltpu.SMEM), held, held, VM],
        out_specs=VM,
        scratch_shapes=[pltpu.SemaphoreType.DMA((2,))],
        compiler_params=pltpu.CompilerParams(vmem_limit_bytes=8 * 1024 * 1024),
        name="packed",
    )(ep, x, y, extra)


def touched_kernel(*refs):
    refs[-1][...] = jnp.zeros_like(refs[-1])


def touched(*arrays):
    return pl.pallas_call(
        touched_kernel,
        out_shape=jax.ShapeDtypeStruct((8, 128), F32),
        in_specs=[VM] * len(arrays),
        out_specs=VM,
        compiler_params=pltpu.CompilerParams(
            vmem_limit_bytes=1024 * 1024, has_side_effects=True
        ),
        name="touched",
    )(*arrays)


STEP = 16


def sums_kernel(plan, count, *refs):
    ins, outs = refs[:count], refs[count:]
    for out, (rows, terms) in zip(outs, plan):
        for r in range(0, rows, STEP):
            total = None
            for i, source, first_row, n in terms:
                if first_row <= r < first_row + n:
                    at = source + r - first_row
                    part = ins[i][at : at + STEP, :].astype(F32)
                    total = part if total is None else total + part
            out[r : r + STEP, :] = total.astype(BF16)


def sums(arrays, plan):
    width = arrays[0].shape[1]
    return pl.pallas_call(
        functools.partial(sums_kernel, plan, len(arrays)),
        out_shape=tuple(jax.ShapeDtypeStruct((rows, width), BF16) for rows, _ in plan),
        in_specs=[VM] * len(arrays),
        out_specs=(VM,) * len(plan),
        compiler_params=pltpu.CompilerParams(vmem_limit_bytes=8 * 1024 * 1024),
        name="sums",
    )(*arrays)


def last_kernel(own, same, other, other_pair, ids_ref, grad_ref, gate_ref):
    total = (own[...].astype(F32) + same[...].astype(F32)) + (
        other[...].astype(F32) + other_pair[...].astype(F32)
    )
    grad_ref[...] = total[:, :D].astype(BF16)
    slot = total[:, D:].T
    gate_ref[...] = sum(
        jnp.where(ids_ref[...] == e, slot[e : e + 1, :], 0.0) for e in range(EXPERTS)
    )


def last(*arrays):
    rows, ids = arrays[0].shape[0], arrays[-1]
    return pl.pallas_call(
        last_kernel,
        out_shape=(
            jax.ShapeDtypeStruct((rows, D), BF16),
            jax.ShapeDtypeStruct(ids.shape, F32),
        ),
        in_specs=[VM] * 5,
        out_specs=(VM, VM),
        compiler_params=pltpu.CompilerParams(vmem_limit_bytes=4 * 1024 * 1024),
        name="last",
    )(*arrays)


NT = (((1,), (1,)), ((), ()))


def expert_kernel(count, held, at, ep_ref, *refs):
    chunks = refs[:count]
    wg_ref, wu_ref, wd_ref = refs[count : count + 3]
    mine_ref, theirs_ref, x_ref, y_ref, coef_ref, cg, cu = refs[count + 3 + held :]
    extra = []
    tokens = cg.shape[0]
    begin = at
    for c in chunks:
        rows = c.shape[0]
        x_ref[at : at + rows, :] = c[:, :D]
        y_ref[at : at + rows, :] = c[:, D : 2 * D]
        extra.append(c[:, 2 * D :].astype(F32))
        at += rows
    xs, ys = x_ref.at[begin:at, :], y_ref.at[begin:at, :]
    coef_ref = coef_ref.at[:, begin:at]
    extra = jnp.concatenate(extra, axis=0).T
    low = ep_ref[0] == 0
    hidden = wg_ref.shape[0] // 2
    gate = lax.dot_general(wg_ref[...], xs[...], NT, preferred_element_type=F32)
    up = lax.dot_general(wu_ref[...], xs[...], NT, preferred_element_type=F32)
    back = lax.dot_general(wd_ref[...], ys[...], NT, preferred_element_type=F32)
    s = 1.0 / (1.0 + jnp.exp(-gate))
    gs = gate * s
    act = gs * up
    product = act * back
    slot_rows = []
    for e in (0, 1):
        mine = slice(e * hidden, (e + 1) * hidden)
        slot_rows.append(jnp.sum(product[mine], axis=0, keepdims=True))
        weight = jnp.where(low, extra[e : e + 1, :], extra[e + 2 : e + 3, :])
        dact = weight * back[mine]
        dgate = dact * up[mine] * s[mine] * (1.0 + gate[mine] * (1.0 - s[mine]))
        coef_ref[e * hidden : (e + 1) * hidden, :] = dgate.astype(BF16)
        coef_ref[(2 + e) * hidden : (3 + e) * hidden, :] = (dact * gs[mine]).astype(BF16)
        coef_ref[(4 + e) * hidden : (5 + e) * hidden, :] = (weight * act[mine]).astype(BF16)
    cg[...] = coef_ref[: 2 * hidden, :].astype(F32).T.astype(BF16)
    cu[...] = coef_ref[2 * hidden : 4 * hidden, :].astype(F32).T.astype(BF16)
    half = tokens // 2

    def column(j, carry):
        cols = pl.ds(pl.multiple_of(j * TILE, TILE), TILE)
        dx = jnp.dot(cg[...], wg_ref[:, cols], preferred_element_type=F32) + jnp.dot(
            cu[...], wu_ref[:, cols], preferred_element_type=F32
        )
        mine_ref[:, cols] = dx[:half].astype(BF16)
        theirs_ref[:, cols] = dx[half:].astype(BF16)
        return carry

    lax.fori_loop(0, D // TILE, column, 0)
    row = lax.broadcasted_iota(jnp.int32, (EXTRA, tokens), 0)
    base = 2 * ep_ref[0]
    slot = jnp.where(row == base, slot_rows[0], 0.0) + jnp.where(row == base + 1, slot_rows[1], 0.0)
    slot = slot.T.astype(BF16)
    mine_ref[:, D:] = slot[:half]
    theirs_ref[:, D:] = slot[half:]


def expert_group(ep, chunks, weights, held, at, total):
    tokens = sum(c.shape[0] for c in chunks)
    hidden2 = weights[0].shape[0]
    part = jax.ShapeDtypeStruct((tokens // 2, D + EXTRA), BF16)
    whole = jax.ShapeDtypeStruct((total, D), BF16)
    before = 1 + len(chunks) + 3
    mine, theirs, *held = pl.pallas_call(
        functools.partial(expert_kernel, len(chunks), len(held), at),
        out_shape=(part, part, whole, whole, jax.ShapeDtypeStruct((3 * hidden2, total), BF16)),
        in_specs=[pl.BlockSpec(memory_space=pltpu.SMEM)] + [VM] * (len(chunks) + 3 + len(held)),
        out_specs=(VM,) * 5,
        scratch_shapes=[pltpu.VMEM((tokens, hidden2), BF16), pltpu.VMEM((tokens, hidden2), BF16)],
        input_output_aliases={before + i: 2 + i for i in range(len(held))},
        cost_estimate=pl.CostEstimate(
            flops=2 * tokens * D * hidden2 * 5,
            bytes_accessed=3 * hidden2 * D * 2 + tokens * 3 * D * 2,
            transcendentals=0,
        ),
        compiler_params=pltpu.CompilerParams(vmem_limit_bytes=8 * 1024 * 1024),
        name="experts",
    )(ep, *chunks, *weights, *held)
    return mine, theirs, held


def weight_kernel(which, side_ref, coef_ref, out_ref):
    h = out_ref.shape[0]
    cols = pl.ds(pl.multiple_of(pl.program_id(0) * TILE, TILE), TILE)
    out_ref[...] = jnp.dot(
        coef_ref[which * h : (which + 1) * h, :], side_ref[:, cols], preferred_element_type=F32
    ).astype(BF16)


def weight_grad(which, side, coef):
    tokens, hidden2 = side.shape[0], coef.shape[0] // 3
    return pl.pallas_call(
        functools.partial(weight_kernel, which),
        grid=(D // TILE,),
        out_shape=jax.ShapeDtypeStruct((hidden2, D), BF16),
        in_specs=[VM, VM],
        out_specs=pl.BlockSpec((hidden2, TILE), lambda j: (0, j)),
        cost_estimate=pl.CostEstimate(
            flops=2 * tokens * D * hidden2,
            bytes_accessed=hidden2 * D * 2 + tokens * D * 2,
            transcendentals=0,
        ),
        compiler_params=pltpu.CompilerParams(vmem_limit_bytes=8 * 1024 * 1024),
        name="weights",
    )(side, coef)


def shards(hidden_in, out_grad, expert_ids, gate_values, w_gate, w_up, w_down):
    local, hidden = w_gate.shape[:2]
    wg, wu, wd = (w.reshape(local * hidden, D) for w in (w_gate, w_up, w_down))
    touched(wg, wu, wd)
    ep = lax.axis_index("ep").astype(jnp.int32).reshape(1)
    experts = lax.broadcasted_iota(jnp.int32, (1, 1, EXTRA), 2)
    chosen = expert_ids[:, :, None] == experts
    weights = jnp.sum(jnp.where(chosen, gate_values[:, :, None], jnp.zeros((), BF16)), axis=1)
    own = packed(ep, hidden_in, out_grad, weights)
    one = own.shape[0]
    two = joined(own, sent(own, OTHER_Y))

    n_a, n_b, n_far = sent(two, first(-1)), sent(two, first(1)), sent(two, first(2))
    near = joined(n_a, n_b, two)
    m_a, m_b = sent(near, second(-1)), sent(near, second(1))
    e_a, e_b = sent(n_far, second(-1)), sent(n_far, second(1))
    k, j = near.shape[0] // 2, n_far.shape[0] // 2
    fm_a, fm_b = sent(taken(m_a, 0, k), second(-1)), sent(taken(m_b, k, k), second(1))
    fe_a, fe_b = sent(taken(e_a, 0, j), second(-1)), sent(taken(e_b, j, j), second(1))

    groups = []
    for group in ((near, n_far), (m_a, e_a), (m_b, e_b), (fm_a, fe_a, fm_b, fe_b)):
        both = [sent(c, OTHER_CORE) for c in group]
        groups.append((*group, *both))

    parts, held, at = {}, (), 0
    tokens = one * X * Z * Y * CORE
    for g in (0, 1, 3, 2):
        group = groups[g]
        mine, theirs, held = expert_group(ep, group, (wg, wu, wd), held, at, tokens)
        at += sum(c.shape[0] for c in group)
        parts[g] = (mine, sent(theirs, OTHER_CORE))
    x_all, y_all, coef_all = held

    h, r = two.shape[0], k + j
    n = 2 * h
    up, down = sums(
        parts[3], tuple((r, ((0, i * r, 0, r), (1, i * r, 0, r))) for i in (0, 1))
    )
    up, down = sent(up, second(1)), sent(down, second(-1))
    line = ((0, 0, 0, n), (1, 0, 0, n), (0, n + h, n, h), (1, n + h, n, h))
    g_a, t_a = sums(
        (*parts[1], up),
        (
            (n + h, (*line, (2, 0, 0, k), (2, k, n, j))),
            (h, ((0, n, 0, h), (1, n, 0, h))),
        ),
    )
    g_b, t_b = sums(
        (*parts[2], down),
        (
            (n + h, (*line, (2, 0, k, n - k), (2, k, n + j, j))),
            (h, ((0, n, 0, h), (1, n, 0, h), (2, n - k, 0, h))),
        ),
    )
    g_a, g_b = sent(g_a, second(1)), sent(g_b, second(-1))
    t_a, t_b = sent(t_a, second(1)), sent(t_b, second(-1))
    n_a, n_b, n_far = sums(
        (*parts[0], g_a, g_b),
        tuple(
            (h, ((0, at, 0, h), (1, at, 0, h), (2, i * h, 0, h), (3, i * h, 0, h)))
            for i, at in enumerate((0, h, 3 * h))
        ),
    )
    n_a, n_b = sent(n_a, first(1)), sent(n_b, first(-1))
    n_far = sent(n_far, first(2))
    own, pair = sums(
        (*parts[0], t_a, t_b, n_a, n_b, n_far),
        tuple(
            (one, tuple((i, a * one + (n if i < 2 else 0), 0, one) for i in range(7)))
            for a in range(2)
        ),
    )
    same = sent(pair, OTHER_Y)
    other, other_pair = sent(own, OTHER_EP), sent(pair, OTHER_BOTH)
    input_grad, gate_grad = last(own, same, other, other_pair, expert_ids.T)
    gate_grad = gate_grad.T

    grads = []
    for which, side in enumerate((x_all, x_all, y_all)):
        grads.append(weight_grad(which, side, coef_all).reshape(local, hidden, D))
    return (input_grad, gate_grad, *grads)


def solution(mesh):
    rows, split = P("blk", None), P("ep", "blk", None)
    return jax.shard_map(
        shards,
        mesh=mesh,
        in_specs=(rows, rows, rows, rows, split, split, split),
        out_specs=(rows, rows, split, split, split),
        check_vma=False,
    )
```
